32 devices in a mesh: rows: 16 (over z, x, core), cols: 2 (over y).
Axes of the slice: x: 2, y: 2, z: 4, core: 2. Of those that a mesh axis runs over, the one named last changes fastest.
Arguments:
- rhs: float32 [8192, 16], P(('rows', 'cols')), may hold values from -6 to 6
- diagonal: float32 [8192], P(('rows', 'cols')), may hold values from 1 to 16
- blocks: float32 [64, 4, 128, 128], P('rows', 'cols'), may hold values from -0.15625 to 0.15625
- block_cols: int32 [64, 4], P('rows', 'cols'), may hold values from 0 to 31
- counts: int32 [64, 2], P('rows', 'cols'), may hold values from 1 to 2
Outputs:
- solution: float32 [8192, 16], P(('rows', 'cols'))
The draws below stay inside these ranges and needn't reach their ends.
Inputs may be any that keep to these rules, and one draw needn't show every extreme that they name: Every entry of block_cols names a block column within its slot's group, from 0 to 31; entries may repeat within a row. `counts`: every count lies between 1 and 2; the slots past the count in a group hold blocks that are not used.
All inputs are finite; a program needn't handle non-finite values.
Results may differ from the reference program's by a relative error of at most 0.0001.
Values sent between devices are 32-bit elements; how exact they have to be, the bound alone decides.
A program may use at most 64 MiB of HBM per device.

```python
import math
import jax
import jax.numpy as jnp
from jax import lax

BS = 128
S = 16
KC = 2
ITERS = 4
PB = 2
NB = 64
N = 8192
KB = 4
NBC = 32
N_COLS = 2


def plant(result, own_key, least, largest):
    shape = result.shape
    spot = [jax.random.randint(jax.random.fold_in(own_key, axis), (), 0, shape[axis]) for axis in range(len(shape))]
    result = result.at[tuple(spot)].set(least)
    longest = shape.index(max(shape))
    spot[longest] = (spot[longest] + 1) % shape[longest]
    return result.at[tuple(spot)].set(largest)


def level_of(stream_key, dims, shards, smallest, top_value):
    def one(dim, parts):
        draws = jax.random.uniform(jax.random.fold_in(jax.random.fold_in(stream_key, 6), dim), (parts,), jnp.float32, smallest / len(shards), top_value / len(shards))
        return jnp.repeat(jnp.exp(draws), dims[dim] // parts).reshape((-1,) + (1,) * (len(dims) - dim - 1))

    gain = one(*shards[0])
    for cut in shards[1:]:
        gain = gain * one(*cut)
    return gain


def noise(own_key, shape, scale, reach, shards=(), held_as=jnp.bfloat16):
    array = jax.random.normal(own_key, shape, jnp.float32) * scale
    if len(shards) > 0:
        array = level_of(own_key, shape, shards, -0.22, 0.18) * array
    return jnp.clip(array, min=-reach, max=reach).astype(held_as)


def setup_inputs(seed: int = 0) -> dict:
    seeds = jax.random.split(jax.random.key(seed), 6)
    return {
        "rhs": noise(seeds[0], (N, S), 1.0, 6.0, ((0, 32),), jnp.float32),
        "diagonal": jnp.clip(jnp.exp(math.log(16.0) - 2.7725887 * jax.random.uniform(seeds[1], (N,), jnp.float32) ** level_of(seeds[1], (N,), ((0, 32),), -0.2, 0.2)), 1.0, 16.0),
        "blocks": noise(seeds[2], (NB, KB, BS, BS), (3 * BS * KB) ** -0.5, 0.15625, ((0, 16), (1, 2)), jnp.float32),
        "block_cols": plant(jax.random.randint(seeds[3], (NB, KB), 0, NBC), jax.random.fold_in(seeds[3], 1), 0, NBC - 1).astype(jnp.int32),
        "counts": plant(jax.random.randint(seeds[4], (NB, N_COLS), 1, KC + 1), jax.random.fold_in(seeds[4], 1), 1, KC).astype(jnp.int32),
    }


def solve_block(matrix, right):
    size = matrix.shape[0]
    joined = jnp.concatenate([matrix, right], axis=1)
    for index in range(size):
        pivot_row = joined[index] / joined[index, index]
        joined = joined - joined[:, index:index + 1] * pivot_row[None, :]
        joined = joined.at[index].set(pivot_row)
    return joined[:, size:]


def gram(left, right):
    return jnp.dot(left.T, right, precision=lax.Precision.HIGHEST)


def times_block(vectors, small):
    return jnp.dot(vectors, small, precision=lax.Precision.HIGHEST)


def reference(rhs, diagonal, blocks, block_cols, counts):
    slot = jnp.arange(KB, dtype=jnp.int32)
    group = slot // KC
    within = slot % KC
    used = (within[None, :] < counts[:, group]).astype(jnp.float32)
    target = (block_cols // PB) * (N_COLS * PB) + group[None, :] * PB + block_cols % PB
    target = target.astype(jnp.int32)

    def apply(vectors):
        tiles = vectors.reshape(NB, BS, S)
        picked = tiles[target] * used[:, :, None, None]
        product = jnp.einsum("bkij,bkjs->bis", blocks, picked, precision=lax.Precision.HIGHEST)
        return diagonal[:, None] * vectors + product.reshape(N, S)

    solution = jnp.zeros_like(rhs)
    residual = rhs
    direction = rhs
    shadow = rhs
    for iteration in range(ITERS):
        image = apply(direction)
        matrix = gram(shadow, image)
        right = gram(shadow, residual)
        alpha = solve_block(matrix, right)
        middle = residual - times_block(image, alpha)
        second = apply(middle)
        omega = jnp.sum(second * middle) / jnp.sum(second * second)
        cross = gram(shadow, second)
        solution = solution + times_block(direction, alpha) + omega * middle
        residual = middle - omega * second
        beta = -solve_block(matrix, cross)
        direction = residual + times_block(direction - omega * image, beta)
    return solution
```

```python
import functools

import jax
import jax.numpy as jnp
from jax import lax
from jax.experimental import pallas as pl
from jax.experimental.pallas import tpu as pltpu
from jax.sharding import PartitionSpec as P

ITERS = 4
MESH = pl.DeviceIdType.MESH
HIGHEST = lax.Precision.HIGHEST
NT = (((1,), (1,)), ((), ()))
NN = (((1,), (0,)), ((), ()))


def dot(left, right, dims=NN):
    return lax.dot_general(left, right, dims, precision=HIGHEST, preferred_element_type=jnp.float32)


def split(x):
    high = x.astype(jnp.bfloat16)
    rest = x - high.astype(jnp.float32)
    mid = rest.astype(jnp.bfloat16)
    low = (rest - mid.astype(jnp.float32)).astype(jnp.bfloat16)
    return high, mid, low


def right_solve(matrix, right):
    size = matrix.shape[0]
    joined = jnp.concatenate([matrix, right], axis=0)
    lane = lax.broadcasted_iota(jnp.int32, joined.shape, 1)
    for index in range(size):
        scaled = joined[:, index : index + 1] / joined[index : index + 1, index : index + 1]
        joined = jnp.where(lane == index, scaled, joined - scaled * joined[index : index + 1, :])
    return joined[size:]


def kernel(
    R, C, cols_ref, counts_ref, rhs_ref, diag_ref, blocks_ref, out_ref,
    gat0, gat1, small, part, outgoing, smallout, weights, resid, direc, image, aresid, prod, seco,
    gsend, grecv, ssend, srecv, psend, precv,
):
    PB, S, width = rhs_ref.shape
    BR, KC = blocks_ref.shape[0], blocks_ref.shape[1]
    r = lax.axis_index("rows")
    c = lax.axis_index("cols")

    gat = (gat0, gat1)

    barrier = pltpu.get_barrier_semaphore()

    def greet_row(d, carry):
        pl.semaphore_signal(barrier, inc=1, device_id=(lax.rem(r + d, R), c), device_id_type=MESH)
        return carry

    lax.fori_loop(1, R, greet_row, 0)
    for d in range(1, C):
        pl.semaphore_signal(barrier, inc=1, device_id=(r, lax.rem(c + d, C)), device_id_type=MESH)

    for b in range(BR):
        for k in range(KC):
            used = k < counts_ref[b, 0]
            block = jnp.where(used, blocks_ref[b, k], 0.0).T
            for s, piece in enumerate(split(block)):
                weights[b, s, k * width : (k + 1) * width, :] = piece

    for j in range(PB):
        gat[0][r, j] = rhs_ref[j]
        resid[j] = rhs_ref[j]
        direc[j] = rhs_ref[j]
        out_ref[j] = jnp.zeros((S, width), jnp.float32)
    gat[0][r, PB] = jnp.zeros((S, width), jnp.float32)

    pl.semaphore_wait(barrier, R - 1 + C - 1)

    def row_copy(p, dst, first, count):
        ref = gat[p].at[r, pl.ds(first, count)]
        return pltpu.make_async_remote_copy(
            src_ref=ref, dst_ref=ref, send_sem=gsend.at[dst], recv_sem=grecv.at[p, r],
            device_id=(dst, c), device_id_type=MESH,
        )

    def send_rows(p, first, count):
        def body(d, carry):
            row_copy(p, lax.rem(r + d, R), first, count).start()
            return carry
        lax.fori_loop(1, R, body, 0)

    def wait_rows(p, first, count):
        def body(d, carry):
            src = lax.rem(r + d, R)
            ref = gat[p].at[src, pl.ds(first, count)]
            pltpu.make_async_remote_copy(
                src_ref=ref, dst_ref=ref, send_sem=gsend.at[src], recv_sem=grecv.at[p, src],
                device_id=(src, c), device_id_type=MESH,
            ).wait_recv()
            return carry
        lax.fori_loop(1, R, body, 0)

    def wait_sent(p, first, count):
        def body(d, carry):
            row_copy(p, lax.rem(r + d, R), first, count).wait_send()
            return carry
        lax.fori_loop(1, R, body, 0)

    def small_copy(p, d):
        dst = lax.rem(c + d, C)
        return pltpu.make_async_remote_copy(
            src_ref=smallout.at[p], dst_ref=small.at[p, d], send_sem=ssend.at[d],
            recv_sem=srecv.at[p, d], device_id=(r, dst), device_id_type=MESH,
        )

    def part_copy(p, d):
        dst = lax.rem(c + d, C)
        return pltpu.make_async_remote_copy(
            src_ref=outgoing.at[p, d], dst_ref=part.at[p, d], send_sem=psend.at[d],
            recv_sem=precv.at[p, d], device_id=(r, dst), device_id_type=MESH,
        )

    def begin_small(p):
        total = gat[p][0, PB]
        for i in range(1, R):
            total = total + gat[p][i, PB]
        smallout[p] = total
        for d in range(1, C):
            small_copy(p, d).start()

    def end_small(p):
        total = smallout[p]
        for d in range(1, C):
            small_copy(p, d).wait()
            total = total + small[p, d]
        return total

    def block_row(p, b):
        picked = []
        for k in range(KC):
            column = cols_ref[b, k]
            picked.append(gat[p][lax.div(column, PB), lax.rem(column, PB)])
        high, mid, low = split(jnp.concatenate(picked, axis=1))
        first = jnp.concatenate([high, mid, low], axis=0)
        a = lax.dot_general(first, weights[b, 0], NN, preferred_element_type=jnp.float32)
        m = lax.dot_general(first[: 2 * S], weights[b, 1], NN, preferred_element_type=jnp.float32)
        z = lax.dot_general(first[:S], weights[b, 2], NN, preferred_element_type=jnp.float32)
        return a[:S] + ((a[S : 2 * S] + m[:S]) + ((a[2 * S :] + m[S:]) + z))

    def begin_parts(p):
        for b in range(BR):
            prod[b] = block_row(p, b)
        for d in range(1, C):
            dst = lax.rem(c + d, C)
            for j in range(PB):
                outgoing[p, d, j] = prod[dst * PB + j]
            part_copy(p, d).start()

    def end_parts(p, j):
        total = diag_ref[j] * gat[p][r, j] + prod[c * PB + j]
        for d in range(1, C):
            total = total + part[p, d, j]
        return total

    def wait_parts(p):
        for d in range(1, C):
            part_copy(p, d).wait()

    blank = jnp.zeros((S, width - 2 * S), jnp.float32)
    eye = (
        lax.broadcasted_iota(jnp.int32, (S, S), 0) == lax.broadcasted_iota(jnp.int32, (S, S), 1)
    ).astype(jnp.float32)

    send_rows(0, 0, PB + 1)
    wait_rows(0, 0, PB + 1)
    begin_parts(0)
    wait_parts(0)
    for j in range(PB):
        value = end_parts(0, j)
        image[j] = value
        aresid[j] = value
    wait_sent(0, 0, PB + 1)

    def first_half(iteration):
        mt = jnp.zeros((S, S), jnp.float32)
        gt = jnp.zeros((S, S), jnp.float32)
        for j in range(PB):
            gat[1][r, j] = image[j]
            mt = mt + dot(image[j], rhs_ref[j], NT)
            gt = gt + dot(resid[j], rhs_ref[j], NT)
        gat[1][r, PB] = jnp.concatenate([mt, gt, blank], axis=1)
        send_rows(1, 0, PB + 1)
        wait_rows(1, 0, PB + 1)
        begin_small(1)
        begin_parts(1)
        total = end_small(1)
        solved = right_solve(total[:, :S], jnp.concatenate([total[:, S : 2 * S], eye], axis=0))
        alpha, inverse = solved[:S], solved[S:]
        wait_parts(1)
        crossing = jnp.zeros((S, S), jnp.float32)
        along = jnp.zeros((S, 1), jnp.float32)
        square = jnp.zeros((S, 1), jnp.float32)
        for j in range(PB):
            moved = end_parts(1, j)
            middle = resid[j] - dot(alpha, image[j])
            second = aresid[j] - dot(alpha, moved)
            out_ref[j] = out_ref[j] + dot(alpha, direc[j])
            resid[j] = middle
            aresid[j] = moved
            seco[j] = second
            crossing = crossing + dot(second, rhs_ref[j], NT)
            along = along + jnp.sum(second * middle, axis=1, keepdims=True)
            square = square + jnp.sum(second * second, axis=1, keepdims=True)
        wait_sent(1, 0, PB + 1)
        for j in range(PB):
            gat[0][r, j] = seco[j]
        wide = (S, S)
        gat[0][r, PB] = jnp.concatenate(
            [crossing, jnp.broadcast_to(along, wide), jnp.broadcast_to(square, wide),
             jnp.zeros((S, width - 3 * S), jnp.float32)], axis=1,
        )
        return inverse

    def omega_of(total):
        sums = jnp.sum(total, axis=0, keepdims=True)
        return sums[:, S : S + 1] / sums[:, 2 * S : 2 * S + 1]

    def iterate(iteration, carry):
        inverse = first_half(iteration)
        send_rows(0, 0, PB + 1)
        wait_rows(0, 0, PB + 1)
        begin_small(0)
        begin_parts(0)
        total = end_small(0)
        omega = omega_of(total)
        beta = -dot(total[:, :S], inverse)
        for j in range(PB):
            middle = resid[j]
            out_ref[j] = out_ref[j] + omega * middle
            residual = middle - omega * seco[j]
            direc[j] = residual + dot(beta, direc[j] - omega * image[j])
            resid[j] = residual
            prod_part = image[j] - omega * aresid[j]
            image[j] = dot(beta, prod_part)
        wait_parts(0)
        for j in range(PB):
            value = seco[j] - omega * end_parts(0, j)
            aresid[j] = value
            image[j] = value + image[j]
        wait_sent(0, 0, PB + 1)
        return carry

    lax.fori_loop(0, ITERS - 1, iterate, 0)
    first_half(ITERS - 1)
    send_rows(0, PB, 1)
    wait_rows(0, PB, 1)
    begin_small(0)
    omega = omega_of(end_small(0))
    for j in range(PB):
        out_ref[j] = out_ref[j] + omega * resid[j]
    wait_sent(0, PB, 1)


def solution(mesh):
    R, C = mesh.shape["rows"], mesh.shape["cols"]

    def per_device(rhs, diagonal, blocks, block_cols, counts):
        width = blocks.shape[2]
        S = rhs.shape[1]
        PB = rhs.shape[0] // width
        BR, KC = blocks.shape[0], blocks.shape[1]
        vector = pltpu.VMEM((PB, S, width), jnp.float32)
        vmem = pl.BlockSpec(memory_space=pltpu.VMEM)
        smem = pl.BlockSpec(memory_space=pltpu.SMEM)
        out = pl.pallas_call(
            functools.partial(kernel, R, C),
            out_shape=jax.ShapeDtypeStruct((PB, S, width), jnp.float32),
            in_specs=[smem, smem, vmem, vmem, vmem],
            out_specs=vmem,
            scratch_shapes=[
                pltpu.VMEM((R, PB + 1, S, width), jnp.float32),
                pltpu.VMEM((R, PB + 1, S, width), jnp.float32),
                pltpu.VMEM((2, C, S, width), jnp.float32),
                pltpu.VMEM((2, C, PB, S, width), jnp.float32),
                pltpu.VMEM((2, C, PB, S, width), jnp.float32),
                pltpu.VMEM((2, S, width), jnp.float32),
                pltpu.VMEM((BR, 3, KC * width, width), jnp.bfloat16),
                vector, vector, vector, vector,
                pltpu.VMEM((BR, S, width), jnp.float32),
                vector,
                pltpu.SemaphoreType.DMA((R,)),
                pltpu.SemaphoreType.DMA((2, R)),
                pltpu.SemaphoreType.DMA((C,)),
                pltpu.SemaphoreType.DMA((2, C)),
                pltpu.SemaphoreType.DMA((C,)),
                pltpu.SemaphoreType.DMA((2, C)),
            ],
            compiler_params=pltpu.CompilerParams(
                collective_id=0, has_side_effects=True, vmem_limit_bytes=48 * 1024 * 1024
            ),
        )(
            block_cols, counts,
            rhs.reshape(PB, width, S).transpose(0, 2, 1),
            diagonal.reshape(PB, 1, width),
            blocks,
        )
        return out.transpose(0, 2, 1).reshape(PB * width, S)

    in_specs = (
        P(("rows", "cols"), None),
        P(("rows", "cols")),
        P("rows", "cols", None, None),
        P("rows", "cols"),
        P("rows", "cols"),
    )
    return jax.shard_map(
        per_device, mesh=mesh, in_specs=in_specs, out_specs=P(("rows", "cols"), None), check_vma=False
    )
```

```python
import functools

import jax
import jax.numpy as jnp
from jax import lax
from jax.experimental import pallas as pl
from jax.experimental.pallas import tpu as pltpu
from jax.sharding import PartitionSpec as P

ITERS = 4
H = 2
TILE = 8
MESH = pl.DeviceIdType.MESH
HIGHEST = lax.Precision.HIGHEST
NT = (((1,), (1,)), ((), ()))
NN = (((1,), (0,)), ((), ()))


def dot(left, right, dims=NN):
    return lax.dot_general(left, right, dims, precision=HIGHEST, preferred_element_type=jnp.float32)


def split(x):
    high = x.astype(jnp.bfloat16)
    rest = x - high.astype(jnp.float32)
    mid = rest.astype(jnp.bfloat16)
    low = (rest - mid.astype(jnp.float32)).astype(jnp.bfloat16)
    return high, mid, low


def right_solve(matrix, right):
    size = matrix.shape[0]
    joined = jnp.concatenate([matrix, right], axis=0)
    lane = lax.broadcasted_iota(jnp.int32, joined.shape, 1)
    for index in range(size):
        scaled = joined[:, index : index + 1] / joined[index : index + 1, index : index + 1]
        joined = jnp.where(lane == index, scaled, joined - scaled * joined[index : index + 1, :])
    return joined[size:]


def kernel(
    R, C, meta_hbm, rhs_hbm, diag_hbm, blocks_hbm, out_ref,
    gat0, gat1, pay, small, part, outgoing, smallout, weights, raw, metav, metas,
    rhs_ref, diag_ref, resid, direc, image, aresid, prod, seco, sums,
    local, mine, theirs, gsend, grecv, ysend, yrecv, ssend, srecv, psend, precv,
):
    PB, S, width = rhs_ref.shape
    BR, KC = raw.shape[1], raw.shape[2]
    RG = R // H
    r = lax.axis_index("rows")
    c = lax.axis_index("cols")
    h = lax.rem(r, H)
    g = lax.div(r, H)
    gat = (gat0, gat1)
    peers = [(dh, d) for dh in range(H) for d in range(C) if (dh, d) != (0, 0)]

    def row_of(d):
        return lax.rem(g + d, RG)

    def peer(dh, d):
        return (g * H + lax.rem(h + dh, H), lax.rem(c + d, C))

    barrier = pltpu.get_barrier_semaphore()

    def greet(d, carry):
        pl.semaphore_signal(barrier, inc=1, device_id=(row_of(d) * H + h, c), device_id_type=MESH)
        return carry

    lax.fori_loop(1, RG, greet, 0)
    for dh, d in peers:
        pl.semaphore_signal(barrier, inc=1, device_id=peer(dh, d), device_id_type=MESH)

    take_rhs = pltpu.make_async_copy(rhs_hbm, rhs_ref, local.at[0])
    take_blocks = pltpu.make_async_copy(blocks_hbm, raw.at[0], local.at[1])
    take_meta = pltpu.make_async_copy(meta_hbm, metav.at[0], local.at[2])
    take_diag = pltpu.make_async_copy(diag_hbm, diag_ref, local.at[3])
    for copy in (take_rhs, take_meta, take_blocks, take_diag):
        copy.start()
    take_rhs.wait()
    for j in range(PB):
        gat0[g, j] = rhs_ref[j]
        resid[j] = rhs_ref[j]
        direc[j] = rhs_ref[j]
        out_ref[j] = jnp.zeros((S, width), jnp.float32)
    take_meta.wait()
    pltpu.make_async_copy(metav.at[0], metas.at[0], local.at[2]).start()
    take_blocks.wait()

    pl.semaphore_wait(barrier, RG - 1 + H * C - 1)

    def row_copy(p, src, dst):
        ref = gat[p].at[src]
        return pltpu.make_async_remote_copy(
            src_ref=ref, dst_ref=ref, send_sem=gsend.at[dst], recv_sem=grecv.at[p, src],
            device_id=(dst * H + h, c), device_id_type=MESH,
        )

    def pay_copy(p, src, dst):
        ref = pay.at[p, src]
        return pltpu.make_async_remote_copy(
            src_ref=ref, dst_ref=ref, send_sem=ysend.at[dst], recv_sem=yrecv.at[p, src],
            device_id=(dst * H + h, c), device_id_type=MESH,
        )

    def each(action):
        def body(d, carry):
            action(row_of(d))
            return carry
        lax.fori_loop(1, RG, body, 0)

    def send(copy, p):
        each(lambda other: copy(p, g, other).start())

    def receive(copy, p):
        each(lambda other: copy(p, other, other).wait_recv())

    def sent(copy, p):
        each(lambda other: copy(p, g, other).wait_send())

    def peer_copy(source, target, send_sem, recv_sem, dh, d):
        return pltpu.make_async_remote_copy(
            src_ref=source, dst_ref=target, send_sem=send_sem, recv_sem=recv_sem,
            device_id=peer(dh, d), device_id_type=MESH,
        )

    def small_copy(p, dh, d):
        e = dh * C + d
        return peer_copy(smallout.at[p], small.at[p, e], ssend.at[e], srecv.at[p, e], dh, d)

    def part_copy(p, dh, d):
        e = dh * C + d
        return peer_copy(outgoing.at[p, e], part.at[p, e], psend.at[e], precv.at[p, e], dh, d)

    def begin_small(p):
        total = pay[p, 0]
        for i in range(1, RG):
            total = total + pay[p, i]
        smallout[p] = total
        for dh, d in peers:
            small_copy(p, dh, d).start()

    def end_small(p):
        total = smallout[p]
        for dh, d in peers:
            small_copy(p, dh, d).wait()
            total = total + small[p, dh * C + d]
        return total

    def block_row(p, hh, b):
        picked = []
        for k in range(KC):
            column = metas[hh, 0, b * KC + k]
            owner = lax.div(lax.div(column, PB), H)
            picked.append(gat[p][owner, lax.rem(column, PB)])
        high, mid, low = split(jnp.concatenate(picked, axis=1))
        first = jnp.concatenate([high, mid, low], axis=0)
        a = lax.dot_general(first, weights[hh, b, 0], NN, preferred_element_type=jnp.float32)
        m = lax.dot_general(first[: 2 * S], weights[hh, b, 1], NN, preferred_element_type=jnp.float32)
        z = lax.dot_general(first[:S], weights[hh, b, 2], NN, preferred_element_type=jnp.float32)
        return a[:S] + ((a[S : 2 * S] + m[:S]) + ((a[2 * S :] + m[S:]) + z))

    def begin_parts(p):
        for hh in range(H):
            for b in range(BR):
                prod[hh, b] = block_row(p, hh, b)
        for dh, d in peers:
            e = dh * C + d
            for j in range(PB):
                outgoing[p, e, j] = prod[dh, lax.rem(c + d, C) * PB + j]
            part_copy(p, dh, d).start()

    def wait_parts(p):
        for dh, d in peers:
            part_copy(p, dh, d).wait()

    def end_parts(p, j):
        total = diag_ref[j] * gat[p][g, j] + prod[0, c * PB + j]
        for dh, d in peers:
            total = total + part[p, dh * C + d, j]
        return total

    def prepare(hh):
        for b in range(BR):
            for k in range(KC):
                column = metas[hh, 0, b * KC + k]
                count = metas[hh, 0, BR * KC + b]
                here = (k < count) & (lax.rem(lax.div(column, PB), H) == h)
                block = jnp.where(here, raw[hh, b, k], 0.0).T
                for s, piece in enumerate(split(block)):
                    weights[hh, b, s, k * width : (k + 1) * width, :] = piece

    send(row_copy, 0)
    swap_meta = peer_copy(metav.at[0], metav.at[1], mine.at[0], theirs.at[0], 1, 0)
    swap_blocks = peer_copy(raw.at[0], raw.at[1], mine.at[1], theirs.at[1], 1, 0)
    swap_meta.start()
    swap_blocks.start()
    pltpu.make_async_copy(metav.at[0], metas.at[0], local.at[2]).wait()
    swap_meta.wait()
    second_meta = pltpu.make_async_copy(metav.at[1], metas.at[1], local.at[2])
    second_meta.start()
    second_meta.wait()

    prepare(0)
    swap_blocks.wait()
    prepare(1)
    take_diag.wait()
    receive(row_copy, 0)
    begin_parts(0)
    wait_parts(0)
    for j in range(PB):
        value = end_parts(0, j)
        image[j] = value
        aresid[j] = value
    sent(row_copy, 0)

    eye = (
        lax.broadcasted_iota(jnp.int32, (S, S), 0) == lax.broadcasted_iota(jnp.int32, (S, S), 1)
    ).astype(jnp.float32)

    def flat(matrix):
        return [matrix[i : i + TILE] for i in range(0, S, TILE)]

    def unflat(total, first):
        count = S // TILE
        return jnp.concatenate(
            [total[:, first + i * S : first + (i + 1) * S] for i in range(count)], axis=0
        )

    def tile(parts):
        used = sum(x.shape[1] for x in parts)
        return jnp.concatenate(parts + [jnp.zeros((TILE, width - used), jnp.float32)], axis=1)

    half = S * (S // TILE)

    def first_half():
        for j in range(PB):
            gat1[g, j] = image[j]
        send(row_copy, 1)
        mt = jnp.zeros((S, S), jnp.float32)
        gt = jnp.zeros((S, S), jnp.float32)
        for j in range(PB):
            mt = mt + dot(image[j], rhs_ref[j], NT)
            gt = gt + dot(resid[j], rhs_ref[j], NT)
        pay[1, g] = tile(flat(mt) + flat(gt))
        send(pay_copy, 1)
        receive(pay_copy, 1)
        begin_small(1)
        receive(row_copy, 1)
        begin_parts(1)
        total = end_small(1)
        solved = right_solve(unflat(total, 0), jnp.concatenate([unflat(total, half), eye], axis=0))
        alpha, inverse = solved[:S], solved[S:]
        for j in range(PB):
            resid[j] = resid[j] - dot(alpha, image[j])
            out_ref[j] = out_ref[j] + dot(alpha, direc[j])
        sent(row_copy, 1)
        sent(pay_copy, 1)
        wait_parts(1)
        for j in range(PB):
            moved = end_parts(1, j)
            second = aresid[j] - dot(alpha, moved)
            aresid[j] = moved
            seco[j] = second
            gat0[g, j] = second
        return inverse

    def offer_second():
        crossing = jnp.zeros((S, S), jnp.float32)
        along = jnp.zeros((S, 1), jnp.float32)
        square = jnp.zeros((S, 1), jnp.float32)
        for j in range(PB):
            second = seco[j]
            crossing = crossing + dot(second, rhs_ref[j], NT)
            along = along + jnp.sum(second * resid[j], axis=1, keepdims=True)
            square = square + jnp.sum(second * second, axis=1, keepdims=True)
        wide = (TILE, S)
        pay[0, g] = tile(
            flat(crossing)
            + [jnp.broadcast_to(sum(flat(along)), wide), jnp.broadcast_to(sum(flat(square)), wide)]
        )
        send(pay_copy, 0)
        receive(pay_copy, 0)
        begin_small(0)

    def omega_of(total):
        line = jnp.sum(total, axis=0, keepdims=True)
        return line[:, half : half + 1] / line[:, half + S : half + S + 1]

    def iterate(iteration, carry):
        inverse = first_half()
        send(row_copy, 0)
        offer_second()
        receive(row_copy, 0)
        begin_parts(0)
        total = end_small(0)
        omega = omega_of(total)
        beta = -dot(unflat(total, 0), inverse)
        for j in range(PB):
            middle = resid[j]
            out_ref[j] = out_ref[j] + omega * middle
            residual = middle - omega * seco[j]
            direc[j] = residual + dot(beta, direc[j] - omega * image[j])
            resid[j] = residual
            sums[j] = seco[j] + dot(beta, image[j] - omega * aresid[j])
        sent(row_copy, 0)
        sent(pay_copy, 0)
        wait_parts(0)
        for j in range(PB):
            moved = omega * end_parts(0, j)
            aresid[j] = seco[j] - moved
            image[j] = sums[j] - moved
        return carry

    lax.fori_loop(0, ITERS - 1, iterate, 0)
    first_half()
    offer_second()
    omega = omega_of(end_small(0))
    for j in range(PB):
        out_ref[j] = out_ref[j] + omega * resid[j]
    sent(pay_copy, 0)


def solution(mesh):
    R, C = mesh.shape["rows"], mesh.shape["cols"]

    def per_device(rhs, diagonal, blocks, block_cols, counts):
        width = blocks.shape[2]
        S = rhs.shape[1]
        PB = rhs.shape[0] // width
        BR, KC = blocks.shape[0], blocks.shape[1]
        RG, E = R // H, H * C
        f32 = jnp.float32
        vector = pltpu.VMEM((PB, S, width), f32)
        hbm = pl.BlockSpec(memory_space=pltpu.HBM)
        vmem = pl.BlockSpec(memory_space=pltpu.VMEM)
        dma = pltpu.SemaphoreType.DMA
        numbers = jnp.concatenate([block_cols.reshape(-1), counts.reshape(-1)])
        meta = jnp.pad(numbers[None, :], ((0, TILE - 1), (0, width - numbers.shape[0])))
        out = pl.pallas_call(
            functools.partial(kernel, R, C),
            out_shape=jax.ShapeDtypeStruct((PB, S, width), f32),
            in_specs=[hbm, hbm, hbm, hbm],
            out_specs=vmem,
            scratch_shapes=[
                pltpu.VMEM((RG, PB, S, width), f32),
                pltpu.VMEM((RG, PB, S, width), f32),
                pltpu.VMEM((2, RG, TILE, width), f32),
                pltpu.VMEM((2, E, TILE, width), f32),
                pltpu.VMEM((2, E, PB, S, width), f32),
                pltpu.VMEM((2, E, PB, S, width), f32),
                pltpu.VMEM((2, TILE, width), f32),
                pltpu.VMEM((H, BR, 3, KC * width, width), jnp.bfloat16),
                pltpu.VMEM((H, BR, KC, width, width), f32),
                pltpu.VMEM((H, TILE, width), jnp.int32),
                pltpu.SMEM((H, TILE, width), jnp.int32),
                vector,
                pltpu.VMEM((PB, 1, width), f32),
                vector, vector, vector, vector,
                pltpu.VMEM((H, BR, S, width), f32),
                vector, vector,
                dma((4,)), dma((2,)), dma((2,)),
                dma((RG,)), dma((2, RG)),
                dma((RG,)), dma((2, RG)),
                dma((E,)), dma((2, E)),
                dma((E,)), dma((2, E)),
            ],
            compiler_params=pltpu.CompilerParams(
                collective_id=0, has_side_effects=True, vmem_limit_bytes=48 * 1024 * 1024
            ),
        )(
            meta,
            rhs.reshape(PB, width, S).transpose(0, 2, 1),
            diagonal.reshape(PB, 1, width),
            blocks,
        )
        return out.transpose(0, 2, 1).reshape(PB * width, S)

    in_specs = (
        P(("rows", "cols"), None),
        P(("rows", "cols")),
        P("rows", "cols", None, None),
        P("rows", "cols"),
        P("rows", "cols"),
    )
    return jax.shard_map(
        per_device, mesh=mesh, in_specs=in_specs, out_specs=P(("rows", "cols"), None), check_vma=False
    )
```

```python
import functools

import jax
import jax.numpy as jnp
from jax import lax
from jax.experimental import pallas as pl
from jax.experimental.pallas import tpu as pltpu
from jax.sharding import PartitionSpec as P

ITERS = 4
H = 2
TILE = 8
MESH = pl.DeviceIdType.MESH
HIGHEST = lax.Precision.HIGHEST
NT = (((1,), (1,)), ((), ()))
NN = (((1,), (0,)), ((), ()))


def dot(left, right, dims=NN):
    return lax.dot_general(left, right, dims, precision=HIGHEST, preferred_element_type=jnp.float32)


def split(x):
    high = x.astype(jnp.bfloat16)
    rest = x - high.astype(jnp.float32)
    mid = rest.astype(jnp.bfloat16)
    low = (rest - mid.astype(jnp.float32)).astype(jnp.bfloat16)
    return high, mid, low


def right_solve(matrix, right):
    size = matrix.shape[0]
    joined = jnp.concatenate([matrix, right], axis=0)
    lane = lax.broadcasted_iota(jnp.int32, joined.shape, 1)
    for index in range(size):
        scaled = joined[:, index : index + 1] / joined[index : index + 1, index : index + 1]
        joined = jnp.where(lane == index, scaled, joined - scaled * joined[index : index + 1, :])
    return joined[size:]


def kernel(
    R, C, cols_hbm, counts_hbm, rhs_hbm, diag_hbm, blocks_hbm, out_ref,
    gat0, gat1, pay, small, smallout, part, outgoing, weights, raw, colsv, countsv, colss, countss,
    rhs_raw, rhs_ref, diag_ref, resid, direc, image, aresid, prod, seco, sums, xs, gram,
    local, mine, theirs, gsend, grecv, ysend, yrecv, ssend, srecv, psend, precv,
):
    PB, S, width = rhs_ref.shape
    BR, KC = raw.shape[1], raw.shape[2]
    RG = R // H
    N = R * C
    r = lax.axis_index("rows")
    c = lax.axis_index("cols")
    h = lax.rem(r, H)
    g = lax.div(r, H)
    gat = (gat0, gat1)
    me = r * C + c
    peers = [(dh, d) for dh in range(H) for d in range(C) if (dh, d) != (0, 0)]

    def wrap(value, count):
        return jnp.where(value >= count, value - count, value)

    groups = [wrap(g + d, RG) for d in range(RG)]
    halves = [wrap(h + d, H) for d in range(H)]
    columns = [wrap(c + d, C) for d in range(C)]
    row_devices = [(groups[d] * H + h, c) for d in range(1, RG)]
    devices = [
        (groups[i] * H + halves[j], columns[k])
        for i in range(RG) for j in range(H) for k in range(C) if (i, j, k) != (0, 0, 0)
    ]

    near = row_devices
    rest = peers
    NP, mine_slot = RG, g

    def peer(dh, d):
        return (g * H + halves[dh], columns[d])

    barrier = pltpu.get_barrier_semaphore()

    for device in devices:
        pl.semaphore_signal(barrier, inc=1, device_id=device, device_id_type=MESH)

    take_rhs = pltpu.make_async_copy(rhs_hbm, rhs_raw, local.at[0])
    take_blocks = pltpu.make_async_copy(blocks_hbm, raw.at[0], local.at[1])
    take_cols = pltpu.make_async_copy(cols_hbm, colsv.at[0], local.at[2])
    take_counts = pltpu.make_async_copy(counts_hbm, countsv.at[0], local.at[4])
    take_diag = pltpu.make_async_copy(diag_hbm, diag_ref, local.at[3])
    for copy in (take_rhs, take_cols, take_counts, take_blocks, take_diag):
        copy.start()
    take_rhs.wait()
    for j in range(PB):
        own = rhs_raw[:, j * width : (j + 1) * width]
        rhs_ref[j] = own
        gat0[g, j] = own
        resid[j] = own
        direc[j] = own
        xs[j] = jnp.zeros((S, width), jnp.float32)

    def to_scalars(i):
        first = pltpu.make_async_copy(colsv.at[i], colss.at[i], local.at[2])
        other = pltpu.make_async_copy(countsv.at[i], countss.at[i], local.at[4])
        first.start()
        other.start()
        first.wait()
        other.wait()

    take_cols.wait()
    take_counts.wait()
    to_scalars(0)
    take_blocks.wait()

    pl.semaphore_wait(barrier, N - 1)

    def broadcast(ref, send_sem, recv_sem, targets):
        for device in targets:
            pltpu.make_async_remote_copy(
                src_ref=ref, dst_ref=ref, send_sem=send_sem, recv_sem=recv_sem,
                device_id=device, device_id_type=MESH,
            ).start()

    def all_of(ref, send_sem, recv_sem):
        return pltpu.make_async_remote_copy(
            src_ref=ref, dst_ref=ref, send_sem=send_sem, recv_sem=recv_sem,
            device_id=row_devices[0], device_id_type=MESH,
        )

    def send(p):
        broadcast(gat[p].at[g], gsend.at[p], grecv.at[p], row_devices)

    def rows_copied(p):
        return all_of(gat[p].at[pl.ds(0, RG - 1)], gsend.at[p], grecv.at[p])

    def receive(p):
        rows_copied(p).wait_recv()

    def sent(p):
        rows_copied(p).wait_send()

    def pay_send(p):
        broadcast(pay.at[p, mine_slot], ysend.at[p], yrecv.at[p], near)

    def pay_copied(p):
        return all_of(pay.at[p, pl.ds(0, NP - 1)], ysend.at[p], yrecv.at[p])

    def pay_sent(p):
        pay_copied(p).wait_send()

    def peer_copy(source, target, send_sem, recv_sem, dh, d):
        return pltpu.make_async_remote_copy(
            src_ref=source, dst_ref=target, send_sem=send_sem, recv_sem=recv_sem,
            device_id=peer(dh, d), device_id_type=MESH,
        )

    def small_copy(p, dh, d):
        e = dh * C + d
        return peer_copy(smallout.at[p], small.at[p, e], ssend.at[e], srecv.at[p, e], dh, d)

    def pay_half(p):
        pay_copied(p).wait_recv()
        values = [pay[p, i] for i in range(NP)]
        while len(values) > 1:
            values = [sum(values[i : i + 2]) for i in range(0, len(values), 2)]
        smallout[p] = values[0]
        for dh, d in rest:
            small_copy(p, dh, d).start()

    def pay_total(p):
        total = smallout[p]
        for dh, d in rest:
            small_copy(p, dh, d).wait()
            total = total + small[p, dh * C + d]
        return total

    def part_copy(p, dh, d):
        e = dh * C + d
        return peer_copy(outgoing.at[p, e], part.at[p, e], psend.at[e], precv.at[p, e], dh, d)

    def block_row(p, hh, b):
        picked = []
        for k in range(KC):
            column = colss[hh, b, k]
            owner = lax.div(lax.div(column, PB), H)
            picked.append(gat[p][owner, lax.rem(column, PB)])
        high, mid, low = split(jnp.concatenate(picked, axis=1))
        first = jnp.concatenate([high, mid, low], axis=0)
        a = lax.dot_general(first, weights[hh, b, 0], NN, preferred_element_type=jnp.float32)
        m = lax.dot_general(first[: 2 * S], weights[hh, b, 1], NN, preferred_element_type=jnp.float32)
        z = lax.dot_general(first[:S], weights[hh, b, 2], NN, preferred_element_type=jnp.float32)
        return a[:S] + ((a[S : 2 * S] + m[:S]) + ((a[2 * S :] + m[S:]) + z))

    def begin_parts(p):
        for dh, d in sorted(peers, key=lambda at: at[1] == 0):
            e = dh * C + d
            for j in range(PB):
                outgoing[p, e, j] = block_row(p, dh, columns[d] * PB + j)
            part_copy(p, dh, d).start()
        for j in range(PB):
            prod[j] = block_row(p, 0, c * PB + j)

    def wait_parts(p):
        for dh, d in peers:
            part_copy(p, dh, d).wait()

    def end_parts(p, j):
        total = diag_ref[j] * gat[p][g, j] + prod[j]
        for dh, d in peers:
            total = total + part[p, dh * C + d, j]
        return total

    def prepare(hh):
        for b in range(BR):
            for k in range(KC):
                column = colss[hh, b, k]
                count = countss[hh, b, 0]
                here = (k < count) & (lax.rem(lax.div(column, PB), H) == h)
                block = jnp.where(here, raw[hh, b, k], 0.0).T
                for s, piece in enumerate(split(block)):
                    weights[hh, b, s, k * width : (k + 1) * width, :] = piece

    send(0)
    swaps = [
        peer_copy(ref.at[0], ref.at[1], mine.at[i], theirs.at[i], 1, 0)
        for i, ref in enumerate((colsv, countsv, raw))
    ]
    for swap in swaps:
        swap.start()
    gram[...] = dot(rhs_raw[...], rhs_raw[...], NT)
    prepare(0)
    for swap in swaps:
        swap.wait()
    to_scalars(1)
    prepare(1)
    take_diag.wait()
    receive(0)
    begin_parts(0)
    wait_parts(0)
    for j in range(PB):
        value = end_parts(0, j)
        image[j] = value
        aresid[j] = value
    sent(0)

    eye = (
        lax.broadcasted_iota(jnp.int32, (S, S), 0) == lax.broadcasted_iota(jnp.int32, (S, S), 1)
    ).astype(jnp.float32)

    def flat(matrix):
        return [matrix[i : i + TILE] for i in range(0, S, TILE)]

    def unflat(total, first):
        count = S // TILE
        return jnp.concatenate(
            [total[:, first + i * S : first + (i + 1) * S] for i in range(count)], axis=0
        )

    def tile(parts):
        used = sum(x.shape[1] for x in parts)
        return jnp.concatenate(parts + [jnp.zeros((TILE, width - used), jnp.float32)], axis=1)

    half = S * (S // TILE)

    def first_half():
        held = [image[j] for j in range(PB)]
        for j in range(PB):
            gat1[g, j] = held[j]
        mt = dot(jnp.concatenate(held, axis=1), rhs_raw[...], NT)
        pay[1, mine_slot] = tile(flat(mt) + flat(gram[...]))
        pay_send(1)
        send(1)
        pay_half(1)
        receive(1)
        begin_parts(1)
        total = pay_total(1)
        solved = right_solve(unflat(total, 0), jnp.concatenate([unflat(total, half), eye], axis=0))
        alpha, inverse = solved[:S], solved[S:]
        for j in range(PB):
            resid[j] = resid[j] - dot(alpha, image[j])
            xs[j] = xs[j] + dot(alpha, direc[j])
        sent(1)
        pay_sent(1)
        wait_parts(1)
        for j in range(PB):
            moved = end_parts(1, j)
            second = aresid[j] - dot(alpha, moved)
            aresid[j] = moved
            seco[j] = second
            gat0[g, j] = second
        return inverse

    def offer_second():
        along = jnp.zeros((S, 1), jnp.float32)
        square = jnp.zeros((S, 1), jnp.float32)
        held = [seco[j] for j in range(PB)]
        crossing = dot(jnp.concatenate(held, axis=1), rhs_raw[...], NT)
        for j in range(PB):
            along = along + jnp.sum(held[j] * resid[j], axis=1, keepdims=True)
            square = square + jnp.sum(held[j] * held[j], axis=1, keepdims=True)
        wide = (TILE, S)
        pay[0, mine_slot] = tile(
            flat(crossing)
            + [jnp.broadcast_to(sum(flat(along)), wide), jnp.broadcast_to(sum(flat(square)), wide)]
        )
        pay_send(0)

    def omega_of(total):
        line = jnp.sum(total, axis=0, keepdims=True)
        return line[:, half : half + 1] / line[:, half + S : half + S + 1]

    def iterate(iteration, carry):
        inverse = first_half()
        offer_second()
        send(0)
        pay_half(0)
        receive(0)
        begin_parts(0)
        total = pay_total(0)
        omega = omega_of(total)
        beta = -dot(unflat(total, 0), inverse)
        for j in range(PB):
            middle = resid[j]
            xs[j] = xs[j] + omega * middle
            residual = middle - omega * seco[j]
            direc[j] = residual + dot(beta, direc[j] - omega * image[j])
            resid[j] = residual
            sums[j] = seco[j] + dot(beta, image[j] - omega * aresid[j])
        gram[...] = dot(jnp.concatenate([resid[j] for j in range(PB)], axis=1), rhs_raw[...], NT)
        sent(0)
        pay_sent(0)
        wait_parts(0)
        for j in range(PB):
            moved = omega * end_parts(0, j)
            aresid[j] = seco[j] - moved
            image[j] = sums[j] - moved
        return carry

    lax.fori_loop(0, ITERS - 1, iterate, 0)
    first_half()
    offer_second()
    pay_half(0)
    omega = omega_of(pay_total(0))
    for j in range(PB):
        out_ref[:, j * width : (j + 1) * width] = xs[j] + omega * resid[j]
    pay_sent(0)


def solution(mesh):
    R, C = mesh.shape["rows"], mesh.shape["cols"]

    def per_device(rhs, diagonal, blocks, block_cols, counts):
        width = blocks.shape[2]
        S = rhs.shape[1]
        PB = rhs.shape[0] // width
        BR, KC = blocks.shape[0], blocks.shape[1]
        RG, E, N = R // H, H * C, R * C
        f32 = jnp.float32
        vector = pltpu.VMEM((PB, S, width), f32)
        hbm = pl.BlockSpec(memory_space=pltpu.HBM)
        vmem = pl.BlockSpec(memory_space=pltpu.VMEM)
        dma = pltpu.SemaphoreType.DMA
        out = pl.pallas_call(
            functools.partial(kernel, R, C),
            out_shape=jax.ShapeDtypeStruct((S, PB * width), f32),
            in_specs=[hbm] * 5,
            out_specs=vmem,
            scratch_shapes=[
                pltpu.VMEM((RG, PB, S, width), f32),
                pltpu.VMEM((RG, PB, S, width), f32),
                pltpu.VMEM((2, RG, TILE, width), f32),
                pltpu.VMEM((2, E, TILE, width), f32),
                pltpu.VMEM((2, TILE, width), f32),
                pltpu.VMEM((2, E, PB, S, width), f32),
                pltpu.VMEM((2, E, PB, S, width), f32),
                pltpu.VMEM((H, BR, 3, KC * width, width), jnp.bfloat16),
                pltpu.VMEM((H, BR, KC, width, width), f32),
                pltpu.VMEM((H, BR, KC), jnp.int32),
                pltpu.VMEM((H, BR, 1), jnp.int32),
                pltpu.SMEM((H, BR, KC), jnp.int32),
                pltpu.SMEM((H, BR, 1), jnp.int32),
                pltpu.VMEM((S, PB * width), f32),
                vector,
                pltpu.VMEM((PB, 1, width), f32),
                vector, vector, vector, vector,
                vector, vector, vector, vector,
                pltpu.VMEM((S, S), f32),
                dma((5,)), dma((3,)), dma((3,)),
                dma((2,)), dma((2,)),
                dma((2,)), dma((2,)),
                dma((E,)), dma((2, E)),
                dma((E,)), dma((2, E)),
            ],
            compiler_params=pltpu.CompilerParams(
                collective_id=0, has_side_effects=True, vmem_limit_bytes=48 * 1024 * 1024
            ),
        )(
            block_cols, counts, rhs.T,
            diagonal.reshape(PB, 1, width),
            blocks,
        )
        return out.T

    in_specs = (
        P(("rows", "cols"), None),
        P(("rows", "cols")),
        P("rows", "cols", None, None),
        P("rows", "cols"),
        P("rows", "cols"),
    )
    return jax.shard_map(
        per_device, mesh=mesh, in_specs=in_specs, out_specs=P(("rows", "cols"), None), check_vma=False
    )
```
